8 devices in a mesh: mat: 2 (over z, y), dp: 4 (over x, core).
Axes of the slice: x: 2, y: 2, z: 1, core: 2. Of those that a mesh axis runs over, the one named last changes fastest.
Arguments:
- a_mat: bfloat16 [4096, 65536], P('mat', 'dp'), parts along dimension 0
Outputs:
- output: float32 [8, 3, 512, 512], P(('mat', 'dp')), parts along dimension 0
There are 2 independent parts. The reference program is written for one: setup_inputs(seed, part) draws one part's arguments, and reference() takes and returns one part's arrays. A program takes and returns all parts, laid end to end along the dimension named above; each array names one.
All inputs are finite; a program needn't handle non-finite values.
Results may differ from the reference program's by a relative error of at most 0.001.
Values are sent between devices in bfloat16 or wider.
A program may use at most 1 GiB of HBM per device.

```python
import jax
import jax.numpy as jnp
from jax import lax

GRAM_ORDER = 2048
COLS_DEV = 16384
GROUPS = 4
MIX_RANK = 8

BLOCK = GRAM_ORDER // GROUPS
SLOTS = GROUPS // 2 + 1
WIDTH = COLS_DEV * GROUPS


def pair_table():
    half = GROUPS // 2
    hi_list = []
    lo_list = []
    for dev_index in range(GROUPS):
        for slot in range(SLOTS):
            other_id = (dev_index - slot) % GROUPS
            if slot < half or dev_index < half:
                hi_list.append(max(dev_index, other_id))
                lo_list.append(min(dev_index, other_id))
            else:
                hi_list.append(-1)
                lo_list.append(-1)
    return jnp.array(hi_list, dtype=jnp.int32), jnp.array(lo_list, dtype=jnp.int32)


def setup_inputs(seed: int = 0, part: int = 0) -> dict:
    key = jax.random.fold_in(jax.random.key(seed), part)
    key_mix, key_src, key_gain = jax.random.split(key, 3)
    mixers = jax.random.normal(key_mix, (GROUPS, GRAM_ORDER, MIX_RANK), jnp.float32) * MIX_RANK ** -0.5
    sources = jax.random.normal(key_src, (GROUPS, MIX_RANK, COLS_DEV), jnp.float32)
    block_gain = jax.random.uniform(key_gain, (GROUPS,), jnp.float32, minval=0.7, maxval=1.4)
    row_gain = jnp.repeat(block_gain, BLOCK)
    mixed = jnp.einsum('snr,srk->nsk', mixers, sources).reshape(GRAM_ORDER, WIDTH)
    scale = (MIX_RANK ** 0.5 / (COLS_DEV * GROUPS ** 0.5)) ** 0.5
    a_mat = mixed * (row_gain[:, None] * scale)
    return {'a_mat': a_mat.astype(jnp.bfloat16)}


def reference(a_mat):
    hi_ids, lo_ids = pair_table()

    def one_block(pair_ids):
        hi_id, lo_id = pair_ids
        hi_rows = lax.dynamic_slice_in_dim(a_mat, jnp.maximum(hi_id, 0) * BLOCK, BLOCK, axis=0)
        lo_rows = lax.dynamic_slice_in_dim(a_mat, jnp.maximum(lo_id, 0) * BLOCK, BLOCK, axis=0)
        block_prod = jnp.dot(hi_rows, lo_rows.T, preferred_element_type=jnp.float32)
        return jnp.where(hi_id >= 0, block_prod, 0.0)

    blocks = lax.map(one_block, (hi_ids, lo_ids))
    return blocks.reshape(GROUPS, SLOTS, BLOCK, BLOCK)
```

```python
import functools

import jax
import jax.numpy as jnp
from jax import lax
from jax.experimental import pallas as pl
from jax.experimental.pallas import tpu as pltpu
from jax.sharding import PartitionSpec as P

BLK = 512
TILE = 256
CHUNK = 2048
DIAG = 3 * TILE
FULL = 4 * TILE

STEPS = (
    dict(diag=True, lhs=(0, 0), rhs=(0, 0), remote=(1, 1), owner=(0, 0), slot=(0, 0)),
    dict(diag=False, lhs=(1, 1), rhs=(0, 0), remote=(1, 1), owner=(1, 1), slot=(1, 1)),
    dict(diag=True, lhs=(1, 1), rhs=(1, 1), remote=(1, 1), owner=(1, 1), slot=(0, 0)),
    dict(diag=False, lhs=(0, 2), rhs=(2, 0), remote=(1, 1), owner=(0, 0), slot=(1, 2)),
    dict(diag=False, lhs=(0, 2), rhs=(2, 0), remote=(0, 1), owner=(0, 0), slot=(2, 1)),
    dict(diag=False, lhs=(1, 2), rhs=(2, 1), remote=(0, 1), owner=(0, 1), slot=(1, 2)),
    dict(diag=True, lhs=(2, 2), rhs=(2, 2), remote=(0, 0), owner=(0, 1), slot=(0, 0)),
    dict(diag=False, lhs=(0, 2), rhs=(2, 0), remote=(0, 0), owner=(1, 1), slot=(1, 1)),
    dict(diag=True, lhs=(0, 0), rhs=(0, 0), remote=(0, 0), owner=(1, 0), slot=(0, 0)),
    dict(diag=False, lhs=(1, 0), rhs=(0, 1), remote=(0, 0), owner=(1, 0), slot=(2, 1)),
)
LOADS = (((2, 0), 0), ((3, 1), 1), ((1, 2), 2), ((0, 3), 2), ((1, 2), 0))
NEEDS = {0: 0, 1: 1, 3: 2, 4: 3, 7: 4}
N_REMOTE = 6


def kernel(a_ref, out_ref, a_buf, part, pair, recv, own, load_sem, d2d_send, d2d_recv, ici_send, ici_recv, out_sem):
    n_chunks = a_ref.shape[1] // CHUNK
    me = lax.axis_index("dp")
    chip = me // 2
    core = me % 2
    peer = chip * 2 + (1 - core)

    def pick(two):
        return two[0] if two[0] == two[1] else two[0] * (1 - chip) + two[1] * chip

    def load(which, c):
        block, slot = LOADS[which]
        return pltpu.make_async_copy(
            a_ref.at[pl.ds(pl.multiple_of(pick(block) * BLK, BLK), BLK), pl.ds(pl.multiple_of(c * CHUNK, CHUNK), CHUNK)],
            a_buf.at[slot * n_chunks + c],
            load_sem.at[which * n_chunks + c],
        )

    for which in range(3):
        for c in range(n_chunks):
            load(which, c).start()

    barrier = pltpu.get_barrier_semaphore()
    for hop in range(1, 4):
        pl.semaphore_signal(barrier, inc=1, device_id={"dp": (me + hop) % 4}, device_id_type=pl.DeviceIdType.MESH)

    def rows_of(s):
        return DIAG if STEPS[s]["diag"] else FULL

    def pair_copy(s):
        half = rows_of(s) // 2
        return pltpu.make_async_remote_copy(
            src_ref=part.at[s % 2, pl.ds(pl.multiple_of((1 - core) * half, 128), half)],
            dst_ref=pair.at[s, pl.ds(0, half)],
            send_sem=d2d_send.at[s],
            recv_sem=d2d_recv.at[s],
            device_id={"dp": peer},
            device_id_type=pl.DeviceIdType.MESH,
        )

    def own_copy(s):
        rows = rows_of(s)
        return pltpu.make_async_remote_copy(
            src_ref=part.at[s % 2, pl.ds(0, rows)],
            dst_ref=own.at[pick(STEPS[s]["slot"]), pl.ds(0, rows)],
            send_sem=d2d_send.at[s],
            recv_sem=d2d_recv.at[s],
            device_id={"dp": peer},
            device_id_type=pl.DeviceIdType.MESH,
        )

    def link_copy(s):
        half = rows_of(s) // 2
        slot = pick(STEPS[s]["slot"])
        return pltpu.make_async_remote_copy(
            src_ref=pair.at[s, pl.ds(0, half)],
            dst_ref=recv.at[slot, pl.ds(pl.multiple_of(core * half, 128), half)],
            send_sem=ici_send.at[s],
            recv_sem=ici_recv.at[slot * 2 + core],
            device_id={"dp": (1 - chip) * 2 + STEPS[s]["owner"][1]},
            device_id_type=pl.DeviceIdType.MESH,
        )

    def link_wait(slot, half_id, half):
        pltpu.make_async_remote_copy(
            src_ref=pair.at[0, pl.ds(0, half)],
            dst_ref=recv.at[slot, pl.ds(half_id * half, half)],
            send_sem=ici_send.at[0],
            recv_sem=ici_recv.at[slot * 2 + half_id],
            device_id={"dp": peer},
            device_id_type=pl.DeviceIdType.MESH,
        ).wait_recv()

    def by_mode(s, remote_fn, own_fn):
        remote = STEPS[s]["remote"]
        if remote == (1, 1):
            remote_fn()
        elif remote == (0, 0):
            own_fn()
        else:
            pl.when(chip == 1)(remote_fn)
            pl.when(chip == 0)(own_fn)

    def after_pop(s):
        is_owner = core == pick(STEPS[s]["owner"])

        def own_fn():
            pl.when(jnp.logical_not(is_owner))(lambda: own_copy(s).start())

        by_mode(s, lambda: pair_copy(s).start(), own_fn)

    def reduce_step(s):
        rows = rows_of(s)
        half = rows // 2
        is_owner = core == pick(STEPS[s]["owner"])

        def remote_fn():
            pair_copy(s).wait()

            @pl.loop(0, half // 128)
            def _(i):
                to = pl.ds(pl.multiple_of(i * 128, 128), 128)
                pair[s, to] += part[s % 2, pl.ds(pl.multiple_of(core * half + i * 128, 128), 128)]

        def own_fn():
            @pl.when(is_owner)
            def _():
                own_copy(s).wait_recv()
                slot = pick(STEPS[s]["slot"])

                @pl.loop(0, rows // 128)
                def _(i):
                    to = pl.ds(pl.multiple_of(i * 128, 128), 128)
                    own[slot, to] += part[s % 2, to]

            @pl.when(jnp.logical_not(is_owner))
            def _():
                own_copy(s).wait_send()

        by_mode(s, remote_fn, own_fn)

    def send_step(s):
        by_mode(s, lambda: link_copy(s).start(), lambda: None)

    def dot(lhs, rhs):
        return lax.dot_general(lhs, rhs, (((1,), (1,)), ((), ())), preferred_element_type=jnp.float32)

    def chunk_body(s, c, first):
        to = part.at[s % 2]
        lhs = a_buf.at[pick(STEPS[s]["lhs"]) * n_chunks + c]
        rhs = a_buf.at[pick(STEPS[s]["rhs"]) * n_chunks + c]
        parts = [(0, lhs[...], rhs[:TILE])]
        if STEPS[s]["diag"]:
            parts.append((BLK, lhs[TILE:], rhs[TILE:]))
        else:
            parts.append((BLK, lhs[...], rhs[TILE:]))
        for at, left, right in parts:
            n = left.shape[0]
            value = dot(left, right)
            to[at:at + n] = value if first else to[at:at + n] + value

    def chunks(s, lo, hi, wait_load):
        if hi - lo == 1:
            last = lo == n_chunks - 1
            if wait_load and not last:
                load(NEEDS[s], lo + 1).wait()
            chunk_body(s, lo, lo == 0)
            if s == 3:
                load(3, lo).start()
            return

        @pl.loop(lo, hi)
        def _(c):
            if wait_load:
                load(NEEDS[s], c + 1).wait()
            chunk_body(s, c, False)
            if s == 3:
                load(3, c).start()

    load(0, 0).wait()
    for s in range(len(STEPS)):
        fresh = s in NEEDS
        if s == 5:
            for c in range(n_chunks):
                load(4, c).start()
        chunks(s, 0, 1, fresh)
        chunks(s, 1, 3, fresh)
        if s == 0:
            pl.semaphore_wait(barrier, 3)
        else:
            reduce_step(s - 1)
        if s + 1 in NEEDS:
            load(NEEDS[s + 1], 0).wait()
        chunks(s, 3, n_chunks - 1, fresh)
        if s > 0:
            send_step(s - 1)
        chunks(s, n_chunks - 1, n_chunks, fresh)
        after_pop(s)

    reduce_step(len(STEPS) - 1)

    for slot in range(3):
        rows = DIAG if slot == 0 else FULL

        def finish(slot=slot, rows=rows):
            for half_id in range(2):
                link_wait(slot, half_id, rows // 2)

            @pl.loop(0, rows // 128)
            def _(i):
                to = pl.ds(pl.multiple_of(i * 128, 128), 128)
                own[slot, to] += recv[slot, to]

        if slot < 2:
            finish()
        else:
            pl.when(chip == 0)(finish)

            @pl.when(chip == 1)
            def _():
                own[2] = jnp.zeros((FULL, TILE), jnp.float32)

    own[0, DIAG:FULL] = own[0, TILE:2 * TILE].T

    def out_copy(slot, at, n, row, col, sem):
        return pltpu.make_async_copy(
            own.at[slot, pl.ds(at, n)], out_ref.at[0, slot, pl.ds(row, n), pl.ds(col, TILE)], out_sem.at[sem]
        )

    copies = [
        out_copy(0, 0, BLK, 0, 0, 0),
        out_copy(0, BLK, TILE, TILE, TILE, 1),
        out_copy(0, DIAG, TILE, 0, TILE, 2),
        out_copy(1, 0, BLK, 0, 0, 3),
        out_copy(1, BLK, BLK, 0, TILE, 4),
        out_copy(2, 0, BLK, 0, 0, 5),
        out_copy(2, BLK, BLK, 0, TILE, 6),
    ]
    for copy in copies:
        copy.start()
    for s in range(N_REMOTE):
        by_mode(s, lambda s=s: link_copy(s).wait_send(), lambda: None)
    for copy in copies:
        copy.wait()


def solution(mesh):
    groups = mesh.shape["dp"]
    assert groups == 4

    def local_gram(a_local):
        n_rows, local_cols = a_local.shape
        assert n_rows == groups * BLK and local_cols % CHUNK == 0
        n_chunks = local_cols // CHUNK
        return pl.pallas_call(
            kernel,
            name="gram",
            out_shape=jax.ShapeDtypeStruct((1, 3, BLK, BLK), jnp.float32),
            in_specs=[pl.BlockSpec(memory_space=pltpu.HBM)],
            out_specs=pl.BlockSpec(memory_space=pltpu.HBM),
            scratch_shapes=[
                pltpu.VMEM((3 * n_chunks, BLK, CHUNK), jnp.bfloat16),
                pltpu.VMEM((2, FULL, TILE), jnp.float32),
                pltpu.VMEM((N_REMOTE, FULL // 2, TILE), jnp.float32),
                pltpu.VMEM((3, FULL, TILE), jnp.float32),
                pltpu.VMEM((3, FULL, TILE), jnp.float32),
                pltpu.SemaphoreType.DMA((len(LOADS) * n_chunks,)),
                pltpu.SemaphoreType.DMA((len(STEPS),)),
                pltpu.SemaphoreType.DMA((len(STEPS),)),
                pltpu.SemaphoreType.DMA((N_REMOTE,)),
                pltpu.SemaphoreType.DMA((6,)),
                pltpu.SemaphoreType.DMA((7,)),
            ],
            compiler_params=pltpu.CompilerParams(
                collective_id=0, has_side_effects=True, vmem_limit_bytes=67043328
            ),
        )(a_local)

    return jax.shard_map(
        local_gram, mesh=mesh, in_specs=(P("mat", "dp"),), out_specs=P(("mat", "dp")), check_vma=False
    )
```

```python
import jax
import jax.numpy as jnp
from jax import lax
from jax.experimental import pallas as pl
from jax.experimental.pallas import tpu as pltpu
from jax.sharding import PartitionSpec as P

BLK = 512
TILE = 256
DHALF = 3 * TILE // 2
MESH = pl.DeviceIdType.MESH

LHS = ((0, 1, 0, 1, 0, 1, 0, 1, 2, 0), (0, 1, 2, 1, 2, 2, 2, 0, 2, 0))
RHS = ((0, 0, 2, 1, 2, 2, 2, 0, 2, 0), (0, 0, 0, 1, 0, 1, 0, 1, 2, 0))
REMOTE = ((1, 1, 1, 1, 0, 0, 0, 0, 0, 0), (1, 1, 1, 1, 1, 1, 0, 0, 0, 0))
OWNER = ((0, 1, 0, 1, 0, 0, 1, 1, 0, 1), (0, 1, 0, 1, 0, 1, 1, 0, 1, 0))
SLOT = ((0, 1, 1, 0, 2, 1, 1, 2, 0, 0), (0, 1, 2, 0, 1, 2, 1, 1, 0, 0))
DIAG = tuple(int(a == b) for a, b in zip(LHS[0], RHS[0]))
N_STEPS = len(DIAG)
LAST = N_STEPS - 1
N_REMOTE = 6
LOADS = (((2, 0), 0), ((3, 1), 1), ((1, 2), 2), ((0, 3), 2), ((1, 2), 0))
FIRST = ((0, 1024), (1024, 2048), (2048, 4096), (4096, 8192), (8192, 12288), (12288, 16384))


def dot(lhs, rhs):
    return lax.dot_general(lhs, rhs, (((1,), (1,)), ((), ())), preferred_element_type=jnp.float32)


def gram_kernel(a_ref, own, a_buf, part, pair, recv, load_sem, d2d_send, d2d_recv, ici_send, ici_recv):
    half_cols = a_ref.shape[1] // 2
    me = lax.axis_index("dp")
    chip = me // 2
    core = me % 2
    peer = chip * 2 + (1 - core)

    def pick(two):
        return two[0] if two[0] == two[1] else two[0] * (1 - chip) + two[1] * chip

    def at(table, s):
        if isinstance(s, int):
            return pick((table[0][s], table[1][s]))
        packed = [sum(v << (2 * i) for i, v in enumerate(row)) for row in table]
        return (pick(packed) >> (2 * s)) & 3

    def load(which, lo, hi, sem):
        block, slot = LOADS[which]
        half = lo // half_cols
        return pltpu.make_async_copy(
            a_ref.at[pl.ds(pl.multiple_of(pick(block) * BLK, BLK), BLK), pl.ds(lo, hi - lo)],
            a_buf.at[slot * 2 + half, :, pl.ds(lo - half * half_cols, hi - lo)],
            load_sem.at[sem],
        )

    first_loads = [load(0, lo, hi, i) for i, (lo, hi) in enumerate(FIRST)]
    half_loads = [
        [load(which, h * half_cols, (h + 1) * half_cols, len(FIRST) + 2 * which + h) for h in range(2)]
        for which in range(1, len(LOADS))
    ]
    for copy in first_loads + half_loads[0] + half_loads[1]:
        copy.start()

    barrier = pltpu.get_barrier_semaphore()
    for hop in range(1, 4):
        pl.semaphore_signal(barrier, inc=1, device_id={"dp": (me + hop) % 4}, device_id_type=MESH)

    part[...] = jnp.zeros_like(part)

    @pl.when(chip == 1)
    def _():
        own[2] = jnp.zeros((2, BLK, TILE), jnp.float32)

    def pair_copy(s):
        return pltpu.make_async_remote_copy(
            src_ref=part.at[s % 2, 1 - core],
            dst_ref=pair.at[s],
            send_sem=d2d_send.at[s],
            recv_sem=d2d_recv.at[s],
            device_id={"dp": peer},
            device_id_type=MESH,
        )

    def own_copy(s, rows):
        return pltpu.make_async_remote_copy(
            src_ref=part.at[s % 2, :, pl.ds(0, rows)],
            dst_ref=own.at[at(SLOT, s), :, pl.ds(0, rows)],
            send_sem=d2d_send.at[s],
            recv_sem=d2d_recv.at[s],
            device_id={"dp": peer},
            device_id_type=MESH,
        )

    def link_copy(s, rows):
        slot = at(SLOT, s)
        return pltpu.make_async_remote_copy(
            src_ref=pair.at[s, pl.ds(0, rows)],
            dst_ref=recv.at[slot, core, pl.ds(0, rows)],
            send_sem=ici_send.at[s],
            recv_sem=ici_recv.at[slot * 2 + core],
            device_id={"dp": (1 - chip) * 2 + at(OWNER, s)},
            device_id_type=MESH,
        )

    def link_wait(slot, half, rows):
        pltpu.make_async_remote_copy(
            src_ref=pair.at[0, pl.ds(0, rows)],
            dst_ref=recv.at[slot, half, pl.ds(0, rows)],
            send_sem=ici_send.at[0],
            recv_sem=ici_recv.at[slot * 2 + half],
            device_id={"dp": peer},
            device_id_type=MESH,
        ).wait_recv()

    def on(value, want=1):
        return pl.when(value == want)

    def send_partial(s):
        @on(at(REMOTE, s))
        def _():
            pair_copy(s).start()

        @on(at(REMOTE, s) * 2 + (at(OWNER, s) + core) % 2)
        def _():
            own_copy(s, BLK).start()

    def reduce_partial(s):
        @on(at(REMOTE, s))
        def _():
            pair_copy(s).wait()

            @pl.loop(0, BLK // 64)
            def _(i):
                rows = pl.ds(pl.multiple_of(i * 64, 64), 64)
                pair[s, rows] += part[s % 2, core, rows]

            for diag, rows in ((1, DHALF), (0, BLK)):
                @on(at((DIAG, DIAG), s), diag)
                def _(rows=rows):
                    link_copy(s, rows).start()

        mine = at(REMOTE, s) * 2 + (at(OWNER, s) + core) % 2

        @on(mine, 0)
        def _():
            own_copy(s, BLK).wait_recv()
            slot = at(SLOT, s)

            @pl.loop(0, BLK // 64)
            def _(i):
                rows = pl.ds(pl.multiple_of(i * 64, 64), 64)
                for h in range(2):
                    own[slot, h, rows] += part[s % 2, h, rows]

        @on(mine, 1)
        def _():
            own_copy(s, BLK).wait_send()

    def put_diag(to, low, high, add):
        for h, row, n, value in (
            (0, 0, DHALF, low[:DHALF]),
            (1, 0, BLK - DHALF, low[DHALF:]),
            (1, BLK - DHALF, TILE, high),
        ):
            to[h, row:row + n] = to[h, row:row + n] + value if add else value

    for i, (lo, hi) in enumerate(FIRST):
        first_loads[i].wait()
        half = lo // half_cols
        cols = slice(lo - half * half_cols, hi - half * half_cols)
        block = a_buf.at[half, :, cols]
        put_diag(part.at[0], dot(block[...], block[:TILE]), dot(block[TILE:], block[TILE:]), i > 0)
    pl.semaphore_wait(barrier, 3)
    send_partial(0)

    @pl.loop(1, 3)
    def _(s):
        @pl.loop(0, 2)
        def _(h):
            @on(s * 2 + h, 2)
            def _():
                half_loads[0][0].wait()

            @on(s * 2 + h, 3)
            def _():
                half_loads[0][1].wait()

            @on(s * 2 + h, 4)
            def _():
                half_loads[1][0].wait()
                half_loads[1][1].wait()

            @on(h)
            def _():
                reduce_partial(s - 1)

            value = dot(a_buf[at(LHS, s) * 2 + h], a_buf[at(RHS, s) * 2 + h])
            for n in range(2):
                old = jnp.where(h == 0, 0.0, part[s % 2, n])
                part[s % 2, n] = old + value[:, n * TILE:(n + 1) * TILE]

        send_partial(s)

    @pl.loop(3, N_STEPS)
    def _(s):
        for step, copies, action in (
            (3, half_loads[2], "start"),
            (4, half_loads[2], "wait"),
            (5, half_loads[3], "start"),
            (6, half_loads[3], "wait"),
        ):
            @on(s, step)
            def _(copies=copies, action=action):
                for copy in copies:
                    getattr(copy, action)()

        diag = at((DIAG, DIAG), s)
        to = part.at[s % 2]
        left, right = at(LHS, s) * 2, at(RHS, s) * 2

        @on(diag)
        def _():
            for h in range(2):
                block = a_buf.at[left + h]
                put_diag(to, dot(block[...], block[:TILE]), dot(block[TILE:], block[TILE:]), h > 0)

        @on(diag, 0)
        def _():
            for h in range(2):
                value = dot(a_buf[left + h], a_buf[right + h])
                for n in range(2):
                    tile = value[:, n * TILE:(n + 1) * TILE]
                    to[n] = to[n] + tile if h else tile

        reduce_partial(s - 1)

        @pl.when(s < LAST)
        def _():
            send_partial(s)

    mine = at(OWNER, LAST) == core
    pl.when(jnp.logical_not(mine))(lambda: own_copy(LAST, DHALF).start())

    def add_link(slot, rows):
        for h in range(2):
            link_wait(slot, h, rows)

        @pl.loop(0, rows // 64)
        def _(i):
            to = pl.ds(pl.multiple_of(i * 64, 64), 64)
            for h in range(2):
                own[slot, h, to] += recv[slot, h, to]

    add_link(1, BLK)
    pl.when(chip == 0)(lambda: add_link(2, BLK))

    @pl.when(mine)
    def _():
        for h in range(2):
            link_wait(0, h, DHALF)

        @pl.loop(0, DHALF // 64)
        def _(i):
            to = pl.ds(pl.multiple_of(i * 64, 64), 64)
            for h in range(2):
                part[LAST % 2, h, to] += recv[0, h, to]

        own_copy(LAST, DHALF).wait_recv()

        @pl.loop(0, DHALF // 64)
        def _(i):
            to = pl.ds(pl.multiple_of(i * 64, 64), 64)
            for h in range(2):
                own[0, h, to] += part[LAST % 2, h, to]

    @pl.when(jnp.logical_not(mine))
    def _():
        add_link(0, DHALF)
        own_copy(LAST, DHALF).wait_send()

    low = jnp.concatenate([own[0, 0, TILE:DHALF], own[0, 1, :BLK - DHALF]], axis=0)
    flipped = low.T
    own[0, 0, DHALF:] = flipped[:BLK - DHALF]
    own[0, 1, DHALF:] = flipped[BLK - DHALF:]

    for s in range(N_REMOTE):
        rows = DHALF if DIAG[s] else BLK

        @on(at(REMOTE, s))
        def _(s=s, rows=rows):
            link_copy(s, rows).wait_send()


def place_kernel(own, out_ref, sem):
    rest = BLK - DHALF
    moves = [
        (0, 0, 0, DHALF, 0, 0),
        (0, 1, 0, rest, DHALF, 0),
        (0, 1, rest, TILE, TILE, TILE),
        (0, 0, DHALF, rest, 0, TILE),
        (0, 1, DHALF, rest, rest, TILE),
    ] + [(slot, h, 0, BLK, 0, h * TILE) for slot in (1, 2) for h in range(2)]
    copies = [
        pltpu.make_async_copy(
            own.at[slot, h, pl.ds(src, n)], out_ref.at[0, slot, pl.ds(row, n), pl.ds(col, TILE)], sem.at[i]
        )
        for i, (slot, h, src, n, row, col) in enumerate(moves)
    ]
    for copy in copies:
        copy.start()
    for copy in copies:
        copy.wait()


def solution(mesh):
    groups = mesh.shape["dp"]
    assert groups == 4

    def local_gram(a_local):
        n_rows, local_cols = a_local.shape
        assert n_rows == groups * BLK and local_cols == FIRST[-1][1]
        own = pl.pallas_call(
            gram_kernel,
            name="gram",
            out_shape=pltpu.VMEM((3, 2, BLK, TILE), jnp.float32),
            in_specs=[pl.BlockSpec(memory_space=pltpu.HBM)],
            out_specs=pl.BlockSpec(memory_space=pltpu.VMEM),
            scratch_shapes=[
                pltpu.VMEM((6, BLK, local_cols // 2), jnp.bfloat16),
                pltpu.VMEM((2, 2, BLK, TILE), jnp.float32),
                pltpu.VMEM((N_REMOTE, BLK, TILE), jnp.float32),
                pltpu.VMEM((3, 2, BLK, TILE), jnp.float32),
                pltpu.SemaphoreType.DMA((len(FIRST) + 2 * len(LOADS),)),
                pltpu.SemaphoreType.DMA((N_STEPS,)),
                pltpu.SemaphoreType.DMA((N_STEPS,)),
                pltpu.SemaphoreType.DMA((N_REMOTE,)),
                pltpu.SemaphoreType.DMA((6,)),
            ],
            compiler_params=pltpu.CompilerParams(
                collective_id=0, has_side_effects=True, vmem_limit_bytes=58 * 2**20
            ),
        )(a_local)
        return pl.pallas_call(
            place_kernel,
            name="place",
            out_shape=jax.ShapeDtypeStruct((1, 3, BLK, BLK), jnp.float32),
            in_specs=[pl.BlockSpec(memory_space=pltpu.VMEM)],
            out_specs=pl.BlockSpec(memory_space=pltpu.HBM),
            scratch_shapes=[pltpu.SemaphoreType.DMA((9,))],
        )(pltpu.with_memory_space_constraint(own, pltpu.VMEM))

    return jax.shard_map(
        local_gram, mesh=mesh, in_specs=(P("mat", "dp"),), out_specs=P(("mat", "dp")), check_vma=False
    )
```

```python
import jax
import jax.numpy as jnp
from jax import lax
from jax.experimental import pallas as pl
from jax.experimental.pallas import tpu as pltpu
from jax.sharding import PartitionSpec as P

BLK = 512
TILE = 256
DHALF = 3 * TILE // 2
MESH = pl.DeviceIdType.MESH

LHS = ((0, 1, 0, 1, 0, 1, 0, 1, 0, 0), (0, 1, 2, 1, 2, 2, 2, 0, 0, 0))
RHS = ((0, 0, 2, 1, 2, 2, 2, 0, 0, 0), (0, 0, 0, 1, 0, 1, 0, 1, 0, 0))
REMOTE = ((1, 1, 1, 1, 0, 0, 0, 0, 0, 0), (1, 1, 1, 1, 1, 1, 0, 0, 0, 0))
OWNER = ((0, 1, 0, 1, 0, 0, 1, 1, 0, 0), (0, 1, 0, 1, 0, 1, 1, 0, 0, 0))
SLOT = ((0, 1, 1, 0, 2, 1, 1, 2, 0, 0), (0, 1, 2, 0, 1, 2, 1, 1, 0, 0))
DIAG = tuple(int(a == b) for a, b in zip(LHS[0], RHS[0]))
N_STEPS = len(DIAG)
LAST = N_STEPS - 1
N_REMOTE = 6
LOADS = (((2, 0), 0), ((3, 1), 1), ((1, 2), 2), ((0, 3), 2), ((1, 2), 0))
FIRST = (((0, 1024),), ((1024, 2816),), ((2816, 5888),), ((5888, 8192), (8192, 10496)), ((10496, 16384),))
FIRST_LOADS = sum(FIRST, ())


def dot(lhs, rhs):
    return lax.dot_general(lhs, rhs, (((1,), (1,)), ((), ())), preferred_element_type=jnp.float32)


def gram_kernel(a_ref, own, a_buf, part, pair, recv, load_sem, d2d_send, d2d_recv, ici_send, ici_recv):
    half_cols = a_ref.shape[1] // 2
    me = lax.axis_index("dp")
    chip = me // 2
    core = me % 2
    peer = chip * 2 + (1 - core)

    def pick(two):
        return two[0] if two[0] == two[1] else two[0] * (1 - chip) + two[1] * chip

    def at(table, s):
        if isinstance(s, int):
            return pick((table[0][s], table[1][s]))
        packed = [sum(v << (2 * i) for i, v in enumerate(row)) for row in table]
        return (pick(packed) >> (2 * s)) & 3

    def operand(table, s):
        last_slots = 2 * ((chip + core + LAST - s) % 2)
        return jnp.where(s < LAST - 1, at(table, s), 0) + jnp.where(s < LAST - 1, 0, 1) * (2 - last_slots)

    def load(which, lo, hi, sem):
        block, slot = LOADS[which]
        half = lo // half_cols
        return pltpu.make_async_copy(
            a_ref.at[pl.ds(pl.multiple_of(pick(block) * BLK, BLK), BLK), pl.ds(lo, hi - lo)],
            a_buf.at[slot * 2 + half, :, pl.ds(lo - half * half_cols, hi - lo)],
            load_sem.at[sem],
        )

    first_loads = [load(0, lo, hi, i) for i, (lo, hi) in enumerate(FIRST_LOADS)]
    half_loads = [
        [load(which, h * half_cols, (h + 1) * half_cols, len(FIRST_LOADS) + 2 * which + h) for h in range(2)]
        for which in range(1, len(LOADS))
    ]
    for copy in first_loads + half_loads[0] + half_loads[1]:
        copy.start()

    barrier = pltpu.get_barrier_semaphore()
    for hop in range(1, 4):
        pl.semaphore_signal(barrier, inc=1, device_id={"dp": (me + hop) % 4}, device_id_type=MESH)

    part[...] = jnp.zeros_like(part)

    @pl.when(chip == 1)
    def _():
        own[2] = jnp.zeros((2, BLK, TILE), jnp.float32)

    def pair_copy(s):
        return pltpu.make_async_remote_copy(
            src_ref=part.at[s % 2, 1 - core],
            dst_ref=pair.at[s],
            send_sem=d2d_send.at[s],
            recv_sem=d2d_recv.at[s],
            device_id={"dp": peer},
            device_id_type=MESH,
        )

    def own_copy(s, rows):
        return pltpu.make_async_remote_copy(
            src_ref=part.at[s % 2, :, pl.ds(0, rows)],
            dst_ref=own.at[at(SLOT, s), :, pl.ds(0, rows)],
            send_sem=d2d_send.at[s],
            recv_sem=d2d_recv.at[s],
            device_id={"dp": peer},
            device_id_type=MESH,
        )

    def link_copy(s, rows):
        slot = at(SLOT, s)
        return pltpu.make_async_remote_copy(
            src_ref=pair.at[s, pl.ds(0, rows)],
            dst_ref=recv.at[slot, core, pl.ds(0, rows)],
            send_sem=ici_send.at[s],
            recv_sem=ici_recv.at[slot * 2 + core],
            device_id={"dp": (1 - chip) * 2 + at(OWNER, s)},
            device_id_type=MESH,
        )

    def link_wait(slot, half, rows):
        pltpu.make_async_remote_copy(
            src_ref=pair.at[0, pl.ds(0, rows)],
            dst_ref=recv.at[slot, half, pl.ds(0, rows)],
            send_sem=ici_send.at[0],
            recv_sem=ici_recv.at[slot * 2 + half],
            device_id={"dp": peer},
            device_id_type=MESH,
        ).wait_recv()

    def on(value, want=1):
        return pl.when(value == want)

    def send_partial(s):
        @on(at(REMOTE, s))
        def _():
            pair_copy(s).start()

        @on(jnp.where(s == LAST - 1, 1, at(REMOTE, s) * 2 + (at(OWNER, s) + core) % 2))
        def _():
            own_copy(s, BLK).start()

    def reduce_partial(s):
        @on(at(REMOTE, s))
        def _():
            pair_copy(s).wait()

            pair[s] += part[s % 2, core]

            for diag, rows in ((1, DHALF), (0, BLK)):
                @on(at((DIAG, DIAG), s), diag)
                def _(rows=rows):
                    link_copy(s, rows).start()

        mine = at(REMOTE, s) * 2 + (at(OWNER, s) + core) % 2

        @on(mine, 0)
        def _():
            own_copy(s, BLK).wait_recv()
            own[at(SLOT, s)] += part[s % 2]

        @on(mine, 1)
        def _():
            own_copy(s, BLK).wait_send()

    def put_diag(to, low, high, add):
        for h, row, n, value in (
            (0, 0, DHALF, low[:DHALF]),
            (1, 0, BLK - DHALF, low[DHALF:]),
            (1, BLK - DHALF, TILE, high),
        ):
            to[h, row:row + n] = to[h, row:row + n] + value if add else value

    arriving = iter(first_loads)
    for i, piece in enumerate(FIRST):
        for _ in piece:
            next(arriving).wait()
        for lo, hi in piece:
            half = lo // half_cols
            block = a_buf.at[half, :, lo - half * half_cols:hi - half * half_cols]
            put_diag(part.at[0], dot(block[...], block[:TILE]), dot(block[TILE:], block[TILE:]), lo > 0)
    pl.semaphore_wait(barrier, 3)
    send_partial(0)

    @pl.loop(1, 3)
    def _(s):
        @pl.loop(0, 2)
        def _(h):
            @on(s * 2 + h, 2)
            def _():
                half_loads[0][0].wait()

            @on(s * 2 + h, 3)
            def _():
                half_loads[0][1].wait()

            @on(s * 2 + h, 4)
            def _():
                half_loads[1][0].wait()
                half_loads[1][1].wait()

            @on(h)
            def _():
                reduce_partial(s - 1)

            value = dot(a_buf[operand(LHS, s) * 2 + h], a_buf[operand(RHS, s) * 2 + h])
            for n in range(2):
                old = jnp.where(h == 0, 0.0, part[s % 2, n])
                part[s % 2, n] = old + value[:, n * TILE:(n + 1) * TILE]

        send_partial(s)

    @pl.loop(3, N_STEPS)
    def _(s):
        for step, copies, action in (
            (3, half_loads[2], "start"),
            (4, half_loads[2], "wait"),
            (5, half_loads[3], "start"),
            (6, half_loads[3], "wait"),
        ):
            @on(s, step)
            def _(copies=copies, action=action):
                for copy in copies:
                    getattr(copy, action)()

        diag = at((DIAG, DIAG), s)
        to = part.at[s % 2]
        left, right = operand(LHS, s) * 2, operand(RHS, s) * 2

        @on(diag)
        def _():
            for h in range(2):
                block = a_buf.at[left + h]
                put_diag(to, dot(block[...], block[:TILE]), dot(block[TILE:], block[TILE:]), h > 0)

        @on(diag, 0)
        def _():
            for h in range(2):
                value = dot(a_buf[left + h], a_buf[right + h])
                for n in range(2):
                    tile = value[:, n * TILE:(n + 1) * TILE]
                    to[n] = to[n] + tile if h else tile

        @pl.when(s < LAST)
        def _():
            reduce_partial(s - 1)
            send_partial(s)

    for h in range(2):
        link_wait(0, h, DHALF)
    own_copy(LAST - 1, BLK).wait()
    for h in range(2):
        own[0, h, :DHALF] += part[LAST % 2, h, :DHALF] + recv[0, h, :DHALF]

    def add_link(slot):
        for h in range(2):
            link_wait(slot, h, BLK)
        own[slot] += recv[slot]

    add_link(1)
    pl.when(chip == 0)(lambda: add_link(2))

    low = jnp.concatenate([own[0, 0, TILE:DHALF], own[0, 1, :BLK - DHALF]], axis=0)
    flipped = low.T
    own[0, 0, DHALF:] = flipped[:BLK - DHALF]
    own[0, 1, DHALF:] = flipped[BLK - DHALF:]

    for s in range(N_REMOTE):
        rows = DHALF if DIAG[s] else BLK

        @on(at(REMOTE, s))
        def _(s=s, rows=rows):
            link_copy(s, rows).wait_send()


def place_kernel(own, out_ref, sem):
    rest = BLK - DHALF
    moves = [
        (0, 0, 0, DHALF, 0, 0),
        (0, 1, 0, rest, DHALF, 0),
        (0, 1, rest, TILE, TILE, TILE),
        (0, 0, DHALF, rest, 0, TILE),
        (0, 1, DHALF, rest, rest, TILE),
    ] + [(slot, h, 0, BLK, 0, h * TILE) for slot in (1, 2) for h in range(2)]
    copies = [
        pltpu.make_async_copy(
            own.at[slot, h, pl.ds(src, n)], out_ref.at[0, slot, pl.ds(row, n), pl.ds(col, TILE)], sem.at[i]
        )
        for i, (slot, h, src, n, row, col) in enumerate(moves)
    ]
    for copy in copies:
        copy.start()
    for copy in copies:
        copy.wait()


def solution(mesh):
    groups = mesh.shape["dp"]
    assert groups == 4

    def local_gram(a_local):
        n_rows, local_cols = a_local.shape
        assert n_rows == groups * BLK and local_cols == FIRST_LOADS[-1][1]
        own = pl.pallas_call(
            gram_kernel,
            name="gram",
            out_shape=pltpu.VMEM((3, 2, BLK, TILE), jnp.float32),
            in_specs=[pl.BlockSpec(memory_space=pltpu.HBM)],
            out_specs=pl.BlockSpec(memory_space=pltpu.VMEM),
            scratch_shapes=[
                pltpu.VMEM((6, BLK, local_cols // 2), jnp.bfloat16),
                pltpu.VMEM((2, 2, BLK, TILE), jnp.float32),
                pltpu.VMEM((N_REMOTE, BLK, TILE), jnp.float32),
                pltpu.VMEM((3, 2, BLK, TILE), jnp.float32),
                pltpu.SemaphoreType.DMA((len(FIRST_LOADS) + 2 * len(LOADS),)),
                pltpu.SemaphoreType.DMA((N_STEPS,)),
                pltpu.SemaphoreType.DMA((N_STEPS,)),
                pltpu.SemaphoreType.DMA((N_REMOTE,)),
                pltpu.SemaphoreType.DMA((6,)),
            ],
            compiler_params=pltpu.CompilerParams(
                collective_id=0, has_side_effects=True, vmem_limit_bytes=60 * 2**20
            ),
        )(a_local)
        return pl.pallas_call(
            place_kernel,
            name="place",
            out_shape=jax.ShapeDtypeStruct((1, 3, BLK, BLK), jnp.float32),
            in_specs=[pl.BlockSpec(memory_space=pltpu.VMEM)],
            out_specs=pl.BlockSpec(memory_space=pltpu.HBM),
            scratch_shapes=[pltpu.SemaphoreType.DMA((9,))],
        )(pltpu.with_memory_space_constraint(own, pltpu.VMEM))

    return jax.shard_map(
        local_gram, mesh=mesh, in_specs=(P("mat", "dp"),), out_specs=P(("mat", "dp")), check_vma=False
    )
```

```python
import jax
import jax.numpy as jnp
from jax import lax
from jax.experimental import pallas as pl
from jax.experimental.pallas import tpu as pltpu
from jax.sharding import PartitionSpec as P

BLK = 512
TILE = 256
DHALF = 3 * TILE // 2
MESH = pl.DeviceIdType.MESH

LHS = ((0, 1, 0, 1, 0, 1, 0, 1, 0, 0), (0, 1, 2, 1, 2, 2, 2, 0, 0, 0))
RHS = ((0, 0, 2, 1, 2, 2, 2, 0, 0, 0), (0, 0, 0, 1, 0, 1, 0, 1, 0, 0))
REMOTE = ((1, 1, 1, 1, 0, 0, 0, 0, 0, 0), (1, 1, 1, 1, 1, 1, 0, 0, 0, 0))
OWNER = ((0, 1, 0, 1, 0, 0, 1, 1, 0, 0), (0, 1, 0, 1, 0, 1, 1, 0, 0, 0))
SLOT = ((0, 1, 1, 0, 2, 1, 1, 2, 0, 0), (0, 1, 2, 0, 1, 2, 1, 1, 0, 0))
DIAG = tuple(int(a == b) for a, b in zip(LHS[0], RHS[0]))
N_STEPS = len(DIAG)
LAST = N_STEPS - 1
N_REMOTE = 6
LOADS = (((2, 0), 0), ((3, 1), 1), ((1, 2), 2), ((0, 3), 2), ((1, 2), 0))
FIRST = (((0, 1024),), ((1024, 3072),), ((3072, 7168),), ((7168, 8192), (8192, 12288)), ((12288, 16384),))
FIRST_LOADS = sum(FIRST, ())


def dot(lhs, rhs):
    return lax.dot_general(lhs, rhs, (((1,), (1,)), ((), ())), preferred_element_type=jnp.float32)


def gram_kernel(a_ref, own, part, recv, a_buf, pair, load_sem, d2d_send, d2d_recv, ici_send, ici_recv):
    half_cols = a_ref.shape[1] // 2
    me = lax.axis_index("dp")
    chip = me // 2
    core = me % 2
    peer = chip * 2 + (1 - core)

    def pick(two):
        return two[0] if two[0] == two[1] else two[0] * (1 - chip) + two[1] * chip

    def at(table, s):
        if isinstance(s, int):
            return pick((table[0][s], table[1][s]))
        packed = [sum(v << (2 * i) for i, v in enumerate(row)) for row in table]
        return (pick(packed) >> (2 * s)) & 3

    def operand(table, s):
        last_slots = 2 * ((chip + core + LAST - s) % 2)
        return jnp.where(s < LAST - 1, at(table, s), 0) + jnp.where(s < LAST - 1, 0, 1) * (2 - last_slots)

    def load(which, lo, hi, sem):
        block, slot = LOADS[which]
        half = lo // half_cols
        return pltpu.make_async_copy(
            a_ref.at[pl.ds(pl.multiple_of(pick(block) * BLK, BLK), BLK), pl.ds(lo, hi - lo)],
            a_buf.at[slot * 2 + half, :, pl.ds(lo - half * half_cols, hi - lo)],
            load_sem.at[sem],
        )

    first_loads = [load(0, lo, hi, i) for i, (lo, hi) in enumerate(FIRST_LOADS)]
    half_loads = [
        [load(which, h * half_cols, (h + 1) * half_cols, len(FIRST_LOADS) + 2 * which + h) for h in range(2)]
        for which in range(1, len(LOADS))
    ]
    for copy in first_loads + half_loads[0] + half_loads[1]:
        copy.start()

    barrier = pltpu.get_barrier_semaphore()
    for hop in range(1, 4):
        pl.semaphore_signal(barrier, inc=1, device_id={"dp": (me + hop) % 4}, device_id_type=MESH)

    part[...] = jnp.zeros_like(part)

    def pair_copy(s):
        return pltpu.make_async_remote_copy(
            src_ref=part.at[s % 2, 1 - core],
            dst_ref=pair.at[s],
            send_sem=d2d_send.at[s],
            recv_sem=d2d_recv.at[s],
            device_id={"dp": peer},
            device_id_type=MESH,
        )

    def own_copy(s, rows):
        return pltpu.make_async_remote_copy(
            src_ref=part.at[s % 2, :, pl.ds(0, rows)],
            dst_ref=own.at[at(SLOT, s), :, pl.ds(0, rows)],
            send_sem=d2d_send.at[s],
            recv_sem=d2d_recv.at[s],
            device_id={"dp": peer},
            device_id_type=MESH,
        )

    def link_copy(s, rows):
        slot = at(SLOT, s)
        return pltpu.make_async_remote_copy(
            src_ref=pair.at[s, pl.ds(0, rows)],
            dst_ref=recv.at[slot, core, pl.ds(0, rows)],
            send_sem=ici_send.at[s],
            recv_sem=ici_recv.at[slot * 2 + core],
            device_id={"dp": (1 - chip) * 2 + at(OWNER, s)},
            device_id_type=MESH,
        )

    def link_wait(slot, half, rows):
        pltpu.make_async_remote_copy(
            src_ref=pair.at[0, pl.ds(0, rows)],
            dst_ref=recv.at[slot, half, pl.ds(0, rows)],
            send_sem=ici_send.at[0],
            recv_sem=ici_recv.at[slot * 2 + half],
            device_id={"dp": peer},
            device_id_type=MESH,
        ).wait_recv()

    def on(value, want=1):
        return pl.when(value == want)

    def send_partial(s):
        @on(at(REMOTE, s))
        def _():
            pair_copy(s).start()

        @on(jnp.where(s == LAST - 1, 1, at(REMOTE, s) * 2 + (at(OWNER, s) + core) % 2))
        def _():
            own_copy(s, BLK).start()

    def reduce_partial(s):
        @on(at(REMOTE, s))
        def _():
            pair_copy(s).wait()

            pair[s] += part[s % 2, core]

            for diag, rows in ((1, DHALF), (0, BLK)):
                @on(at((DIAG, DIAG), s), diag)
                def _(rows=rows):
                    link_copy(s, rows).start()

        mine = at(REMOTE, s) * 2 + (at(OWNER, s) + core) % 2

        @on(mine, 0)
        def _():
            own_copy(s, BLK).wait_recv()
            own[at(SLOT, s)] += part[s % 2]

        @on(mine, 1)
        def _():
            own_copy(s, BLK).wait_send()

    def put_diag(to, low, high, add):
        for h, row, n, value in (
            (0, 0, DHALF, low[:DHALF]),
            (1, 0, BLK - DHALF, low[DHALF:]),
            (1, BLK - DHALF, TILE, high),
        ):
            to[h, row:row + n] = to[h, row:row + n] + value if add else value

    arriving = iter(first_loads)
    for i, piece in enumerate(FIRST):
        for _ in piece:
            next(arriving).wait()
        for lo, hi in piece:
            half = lo // half_cols
            block = a_buf.at[half, :, lo - half * half_cols:hi - half * half_cols]
            put_diag(part.at[0], dot(block[...], block[:TILE]), dot(block[TILE:], block[TILE:]), lo > 0)
    pl.semaphore_wait(barrier, 3)
    send_partial(0)

    @pl.loop(1, 2)
    def _(s):
        @pl.loop(0, 2)
        def _(h):
            @on(s * 2 + h, 2)
            def _():
                half_loads[0][0].wait()

            @on(s * 2 + h, 3)
            def _():
                half_loads[0][1].wait()

            @on(h)
            def _():
                reduce_partial(s - 1)

            value = dot(a_buf[operand(LHS, s) * 2 + h], a_buf[operand(RHS, s) * 2 + h])
            for n in range(2):
                old = jnp.where(h == 0, 0.0, part[s % 2, n])
                part[s % 2, n] = old + value[:, n * TILE:(n + 1) * TILE]

        send_partial(s)

    @pl.loop(2, N_STEPS)
    def _(s):
        for step, copies, action in (
            (2, half_loads[1], "wait"),
            (3, half_loads[2], "start"),
            (4, half_loads[2], "wait"),
            (5, half_loads[3], "start"),
            (6, half_loads[3], "wait"),
        ):
            @on(s, step)
            def _(copies=copies, action=action):
                for copy in copies:
                    getattr(copy, action)()

        diag = at((DIAG, DIAG), s)
        to = part.at[s % 2]
        left, right = operand(LHS, s) * 2, operand(RHS, s) * 2

        @on(diag)
        def _():
            for h in range(2):
                block = a_buf.at[left + h]
                put_diag(to, dot(block[...], block[:TILE]), dot(block[TILE:], block[TILE:]), h > 0)

        @on(diag, 0)
        def _():
            for h in range(2):
                value = dot(a_buf[left + h], a_buf[right + h])
                for n in range(2):
                    tile = value[:, n * TILE:(n + 1) * TILE]
                    to[n] = to[n] + tile if h else tile

        @pl.when(s < LAST)
        def _():
            reduce_partial(s - 1)
            send_partial(s)

    own_copy(LAST - 1, BLK).wait()
    for h in range(2):
        link_wait(0, h, DHALF)
        link_wait(1, h, BLK)

    @pl.when(chip == 0)
    def _():
        for h in range(2):
            link_wait(2, h, BLK)

    for s in range(N_REMOTE):
        rows = DHALF if DIAG[s] else BLK

        @on(at(REMOTE, s))
        def _(s=s, rows=rows):
            link_copy(s, rows).wait_send()


def place_kernel(own, part, recv, out_ref, done, sem):
    chip = lax.axis_index("dp") // 2
    rest = BLK - DHALF
    copies = []

    def move(slot, h, src, n, row, col):
        i = len(copies)
        copies.append(
            pltpu.make_async_copy(
                done.at[slot, h, pl.ds(src, n)], out_ref.at[0, slot, pl.ds(row, n), pl.ds(col, TILE)], sem.at[i]
            )
        )
        copies[i].start()

    def diag_sum(h, row, n):
        return own[0, h, row:row + n] + part[LAST % 2, h, row:row + n] + recv[0, h, row:row + n]

    low = [diag_sum(0, TILE, DHALF - TILE), diag_sum(1, 0, rest)]
    done[0, 0, TILE:DHALF] = low[0]
    done[0, 1, :rest] = low[1]
    done[0, 0, :TILE] = diag_sum(0, 0, TILE)
    move(0, 0, 0, DHALF, 0, 0)
    move(0, 1, 0, rest, DHALF, 0)
    done[0, 1, rest:DHALF] = diag_sum(1, rest, TILE)
    move(0, 1, rest, TILE, TILE, TILE)
    flipped = jnp.concatenate(low, axis=0).T
    done[0, 0, DHALF:] = flipped[:rest]
    done[0, 1, DHALF:] = flipped[rest:]
    move(0, 0, DHALF, rest, 0, TILE)
    move(0, 1, DHALF, rest, rest, TILE)
    for h in range(2):
        done[1, h] = own[1, h] + recv[1, h]
        move(1, h, 0, BLK, 0, h * TILE)
    for h in range(2):
        done[2, h] = jnp.where(chip == 0, own[2, h] + recv[2, h], 0.0)
        move(2, h, 0, BLK, 0, h * TILE)
    for copy in copies:
        copy.wait()


def solution(mesh):
    groups = mesh.shape["dp"]
    assert groups == 4

    def local_gram(a_local):
        n_rows, local_cols = a_local.shape
        assert n_rows == groups * BLK and local_cols == FIRST_LOADS[-1][1]
        sums = pl.pallas_call(
            gram_kernel,
            name="gram",
            out_shape=[pltpu.VMEM((n, 2, BLK, TILE), jnp.float32) for n in (3, 2, 3)],
            in_specs=[pl.BlockSpec(memory_space=pltpu.HBM)],
            out_specs=[pl.BlockSpec(memory_space=pltpu.VMEM)] * 3,
            scratch_shapes=[
                pltpu.VMEM((6, BLK, local_cols // 2), jnp.bfloat16),
                pltpu.VMEM((N_REMOTE, BLK, TILE), jnp.float32),
                pltpu.SemaphoreType.DMA((len(FIRST_LOADS) + 2 * len(LOADS),)),
                pltpu.SemaphoreType.DMA((N_STEPS,)),
                pltpu.SemaphoreType.DMA((N_STEPS,)),
                pltpu.SemaphoreType.DMA((N_REMOTE,)),
                pltpu.SemaphoreType.DMA((6,)),
            ],
            compiler_params=pltpu.CompilerParams(
                collective_id=0, has_side_effects=True, vmem_limit_bytes=55 * 2**20
            ),
        )(a_local)
        return pl.pallas_call(
            place_kernel,
            name="place",
            out_shape=jax.ShapeDtypeStruct((1, 3, BLK, BLK), jnp.float32),
            in_specs=[pl.BlockSpec(memory_space=pltpu.VMEM)] * 3,
            out_specs=pl.BlockSpec(memory_space=pltpu.HBM),
            scratch_shapes=[pltpu.VMEM((3, 2, BLK, TILE), jnp.float32), pltpu.SemaphoreType.DMA((9,))],
            compiler_params=pltpu.CompilerParams(vmem_limit_bytes=8 * 2**20),
        )(*[pltpu.with_memory_space_constraint(x, pltpu.VMEM) for x in sums])

    return jax.shard_map(
        local_gram, mesh=mesh, in_specs=(P("mat", "dp"),), out_specs=P(("mat", "dp")), check_vma=False
    )
```

```python
import jax
import jax.numpy as jnp
from jax import lax
from jax.experimental import pallas as pl
from jax.experimental.pallas import tpu as pltpu
from jax.sharding import PartitionSpec as P

BLK = 512
TILE = 256
DHALF = 3 * TILE // 2
MESH = pl.DeviceIdType.MESH

LHS = ((0, 1, 0, 1, 0, 1, 0, 1, 0, 0), (0, 1, 2, 1, 2, 2, 2, 0, 0, 0))
RHS = ((0, 0, 2, 1, 2, 2, 2, 0, 0, 0), (0, 0, 0, 1, 0, 1, 0, 1, 0, 0))
REMOTE = ((1, 1, 1, 1, 0, 0, 0, 0, 0, 0), (1, 1, 1, 1, 1, 1, 0, 0, 0, 0))
OWNER = ((0, 1, 0, 1, 0, 0, 1, 1, 0, 0), (0, 1, 0, 1, 0, 1, 1, 0, 0, 0))
SLOT = ((0, 1, 1, 0, 2, 1, 1, 2, 0, 0), (0, 1, 2, 0, 1, 2, 1, 1, 0, 0))
DIAG = tuple(int(a == b) for a, b in zip(LHS[0], RHS[0]))
N_STEPS = len(DIAG)
LAST = N_STEPS - 1
N_REMOTE = 6
LOADS = (((2, 0), 0), ((3, 1), 1), ((1, 2), 2), ((0, 3), 2), ((1, 2), 0))
FIRST = ((2, 1024), (1, 2048), (3, 4096))
N_FIRST = sum(n for n, _ in FIRST)

def dot(lhs, rhs):
    return lax.dot_general(lhs, rhs, (((1,), (1,)), ((), ())), preferred_element_type=jnp.float32)


def gram_kernel(a_ref, own, part, recv, a_buf, pair, load_sem, d2d_send, d2d_recv, ici_send, ici_recv):
    half_cols = a_ref.shape[1] // 2
    me = lax.axis_index("dp")
    chip = me // 2
    core = me % 2
    peer = chip * 2 + (1 - core)

    def pick(two):
        return two[0] if two[0] == two[1] else two[0] * (1 - chip) + two[1] * chip

    def at(table, s):
        if isinstance(s, int):
            return pick((table[0][s], table[1][s]))
        packed = [sum(v << (2 * i) for i, v in enumerate(row)) for row in table]
        return (pick(packed) >> (2 * s)) & 3

    def operand(table, s):
        last_slots = 2 * ((chip + core + LAST - s) % 2)
        return jnp.where(s < LAST - 1, at(table, s), 0) + jnp.where(s < LAST - 1, 0, 1) * (2 - last_slots)

    def load(which, lo, hi, sem):
        block, slot = LOADS[which]
        half = lo // half_cols
        return pltpu.make_async_copy(
            a_ref.at[pl.ds(pl.multiple_of(pick(block) * BLK, BLK), BLK), pl.ds(lo, hi - lo)],
            a_buf.at[slot * 2 + half, :, pl.ds(lo - half * half_cols, hi - lo)],
            load_sem.at[sem],
        )

    def first_load(base, width, c):
        col = pl.multiple_of(base + c * width, width)
        cols = pl.ds(pl.multiple_of(col % half_cols, width), width)
        return col // half_cols, cols, pl.ds(col, width)

    segments = []
    for n, width in FIRST:
        done = sum(m for m, _, _ in segments)
        base = sum(m * w for m, w, _ in segments)
        segments.append((n, width, (base, done)))

    def first_copy(width, start, c):
        half, cols, src = first_load(start[0], width, c)
        return pltpu.make_async_copy(
            a_ref.at[pl.ds(pl.multiple_of(pick(LOADS[0][0]) * BLK, BLK), BLK), src],
            a_buf.at[LOADS[0][1] * 2 + half, :, cols],
            load_sem.at[start[1] + c],
        )

    half_loads = [
        [load(which, h * half_cols, (h + 1) * half_cols, N_FIRST + 2 * which + h) for h in range(2)]
        for which in range(1, len(LOADS))
    ]
    for n, width, start in segments:
        for c in range(n):
            first_copy(width, start, c).start()
    for copy in half_loads[0] + half_loads[1]:
        copy.start()

    barrier = pltpu.get_barrier_semaphore()
    for hop in range(1, 4):
        pl.semaphore_signal(barrier, inc=1, device_id={"dp": (me + hop) % 4}, device_id_type=MESH)

    part[...] = jnp.zeros_like(part)

    def pair_copy(s):
        return pltpu.make_async_remote_copy(
            src_ref=part.at[s % 2, 1 - core],
            dst_ref=pair.at[s],
            send_sem=d2d_send.at[s],
            recv_sem=d2d_recv.at[s],
            device_id={"dp": peer},
            device_id_type=MESH,
        )

    def own_copy(s, rows):
        return pltpu.make_async_remote_copy(
            src_ref=part.at[s % 2, :, pl.ds(0, rows)],
            dst_ref=own.at[at(SLOT, s), :, pl.ds(0, rows)],
            send_sem=d2d_send.at[s],
            recv_sem=d2d_recv.at[s],
            device_id={"dp": peer},
            device_id_type=MESH,
        )

    def link_copy(s, rows):
        slot = at(SLOT, s)
        return pltpu.make_async_remote_copy(
            src_ref=pair.at[s, pl.ds(0, rows)],
            dst_ref=recv.at[slot, core, pl.ds(0, rows)],
            send_sem=ici_send.at[s],
            recv_sem=ici_recv.at[slot * 2 + core],
            device_id={"dp": (1 - chip) * 2 + at(OWNER, s)},
            device_id_type=MESH,
        )

    def link_wait(slot, half, rows):
        pltpu.make_async_remote_copy(
            src_ref=pair.at[0, pl.ds(0, rows)],
            dst_ref=recv.at[slot, half, pl.ds(0, rows)],
            send_sem=ici_send.at[0],
            recv_sem=ici_recv.at[slot * 2 + half],
            device_id={"dp": peer},
            device_id_type=MESH,
        ).wait_recv()

    def on(value, want=1):
        return pl.when(value == want)

    def send_partial(s):
        @on(at(REMOTE, s))
        def _():
            pair_copy(s).start()

        @on(jnp.where(s == LAST - 1, 1, at(REMOTE, s) * 2 + (at(OWNER, s) + core) % 2))
        def _():
            own_copy(s, BLK).start()

    def reduce_partial(s):
        @on(at(REMOTE, s))
        def _():
            pair_copy(s).wait()

            pair[s] += part[s % 2, core]

            for diag, rows in ((1, DHALF), (0, BLK)):
                @on(at((DIAG, DIAG), s), diag)
                def _(rows=rows):
                    link_copy(s, rows).start()

        mine = at(REMOTE, s) * 2 + (at(OWNER, s) + core) % 2

        @on(mine, 0)
        def _():
            own_copy(s, BLK).wait_recv()
            own[at(SLOT, s)] += part[s % 2]

        @on(mine, 1)
        def _():
            own_copy(s, BLK).wait_send()

    def put_diag(to, low, high, add):
        for h, row, n, value in (
            (0, 0, DHALF, low[:DHALF]),
            (1, 0, BLK - DHALF, low[DHALF:]),
            (1, BLK - DHALF, TILE, high),
        ):
            to[h, row:row + n] = to[h, row:row + n] + value if add else value

    for n, width, start in segments:
        @pl.loop(0, n)
        def _(c, width=width, start=start):
            first_copy(width, start, c).wait()
            half, cols, _ = first_load(start[0], width, c)
            block = a_buf.at[half, :, cols]
            put_diag(part.at[0], dot(block[...], block[:TILE]), dot(block[TILE:], block[TILE:]), True)

    pl.semaphore_wait(barrier, 3)
    send_partial(0)

    @pl.loop(1, 2)
    def _(s):
        @pl.loop(0, 2)
        def _(h):
            @on(s * 2 + h, 2)
            def _():
                half_loads[0][0].wait()

            @on(s * 2 + h, 3)
            def _():
                half_loads[0][1].wait()

            @on(h)
            def _():
                reduce_partial(s - 1)

            value = dot(a_buf[operand(LHS, s) * 2 + h], a_buf[operand(RHS, s) * 2 + h])
            for n in range(2):
                old = jnp.where(h == 0, 0.0, part[s % 2, n])
                part[s % 2, n] = old + value[:, n * TILE:(n + 1) * TILE]

        send_partial(s)

    @pl.loop(2, N_STEPS)
    def _(s):
        for step, copies, action in (
            (2, half_loads[1], "wait"),
            (3, half_loads[2], "start"),
            (4, half_loads[2], "wait"),
            (5, half_loads[3], "start"),
            (6, half_loads[3], "wait"),
        ):
            @on(s, step)
            def _(copies=copies, action=action):
                for copy in copies:
                    getattr(copy, action)()

        diag = at((DIAG, DIAG), s)
        to = part.at[s % 2]
        left, right = operand(LHS, s) * 2, operand(RHS, s) * 2

        @on(diag)
        def _():
            for h in range(2):
                block = a_buf.at[left + h]
                put_diag(to, dot(block[...], block[:TILE]), dot(block[TILE:], block[TILE:]), h > 0)

        @on(diag, 0)
        def _():
            for h in range(2):
                value = dot(a_buf[left + h], a_buf[right + h])
                for n in range(2):
                    tile = value[:, n * TILE:(n + 1) * TILE]
                    to[n] = to[n] + tile if h else tile

        @pl.when(s < LAST)
        def _():
            reduce_partial(s - 1)
            send_partial(s)

    own_copy(LAST - 1, BLK).wait()
    for h in range(2):
        link_wait(0, h, DHALF)
        link_wait(1, h, BLK)

    @pl.when(chip == 0)
    def _():
        for h in range(2):
            link_wait(2, h, BLK)

    for s in range(N_REMOTE):
        rows = DHALF if DIAG[s] else BLK

        @on(at(REMOTE, s))
        def _(s=s, rows=rows):
            link_copy(s, rows).wait_send()


def place_kernel(own, part, recv, out_ref, done, sem):
    chip = lax.axis_index("dp") // 2
    rest = BLK - DHALF
    copies = []

    def move(slot, h, src, n, row, col):
        i = len(copies)
        copies.append(
            pltpu.make_async_copy(
                done.at[slot, h, pl.ds(src, n)], out_ref.at[0, slot, pl.ds(row, n), pl.ds(col, TILE)], sem.at[i]
            )
        )
        copies[i].start()

    def diag_sum(h, row, n):
        return own[0, h, row:row + n] + part[LAST % 2, h, row:row + n] + recv[0, h, row:row + n]

    low = [diag_sum(0, TILE, DHALF - TILE), diag_sum(1, 0, rest)]
    done[0, 0, TILE:DHALF] = low[0]
    done[0, 1, :rest] = low[1]
    done[0, 0, :TILE] = diag_sum(0, 0, TILE)
    move(0, 0, 0, DHALF, 0, 0)
    move(0, 1, 0, rest, DHALF, 0)
    done[0, 1, rest:DHALF] = diag_sum(1, rest, TILE)
    move(0, 1, rest, TILE, TILE, TILE)
    flipped = jnp.concatenate(low, axis=0).T
    done[0, 0, DHALF:] = flipped[:rest]
    done[0, 1, DHALF:] = flipped[rest:]
    move(0, 0, DHALF, rest, 0, TILE)
    move(0, 1, DHALF, rest, rest, TILE)
    for h in range(2):
        done[1, h] = own[1, h] + recv[1, h]
        move(1, h, 0, BLK, 0, h * TILE)
    for h in range(2):
        done[2, h] = jnp.where(chip == 0, own[2, h] + recv[2, h], 0.0)
        move(2, h, 0, BLK, 0, h * TILE)
    for copy in copies:
        copy.wait()


def solution(mesh):
    groups = mesh.shape["dp"]
    assert groups == 4

    def local_gram(a_local):
        n_rows, local_cols = a_local.shape
        assert n_rows == groups * BLK and local_cols == sum(n * width for n, width in FIRST)
        sums = pl.pallas_call(
            gram_kernel,
            name="gram",
            out_shape=[pltpu.VMEM((n, 2, BLK, TILE), jnp.float32) for n in (3, 2, 3)],
            in_specs=[pl.BlockSpec(memory_space=pltpu.HBM)],
            out_specs=[pl.BlockSpec(memory_space=pltpu.VMEM)] * 3,
            scratch_shapes=[
                pltpu.VMEM((6, BLK, local_cols // 2), jnp.bfloat16),
                pltpu.VMEM((N_REMOTE, BLK, TILE), jnp.float32),
                pltpu.SemaphoreType.DMA((N_FIRST + 2 * len(LOADS),)),
                pltpu.SemaphoreType.DMA((N_STEPS,)),
                pltpu.SemaphoreType.DMA((N_STEPS,)),
                pltpu.SemaphoreType.DMA((N_REMOTE,)),
                pltpu.SemaphoreType.DMA((6,)),
            ],
            compiler_params=pltpu.CompilerParams(
                collective_id=0, has_side_effects=True, vmem_limit_bytes=55 * 2**20
            ),
        )(a_local)
        return pl.pallas_call(
            place_kernel,
            name="place",
            out_shape=jax.ShapeDtypeStruct((1, 3, BLK, BLK), jnp.float32),
            in_specs=[pl.BlockSpec(memory_space=pltpu.VMEM)] * 3,
            out_specs=pl.BlockSpec(memory_space=pltpu.HBM),
            scratch_shapes=[pltpu.VMEM((3, 2, BLK, TILE), jnp.float32), pltpu.SemaphoreType.DMA((9,))],
            compiler_params=pltpu.CompilerParams(vmem_limit_bytes=8 * 2**20),
        )(*[pltpu.with_memory_space_constraint(x, pltpu.VMEM) for x in sums])

    return jax.shard_map(
        local_gram, mesh=mesh, in_specs=(P("mat", "dp"),), out_specs=P(("mat", "dp")), check_vma=False
    )
```

```python
import jax
import jax.numpy as jnp
from jax import lax
from jax.experimental import pallas as pl
from jax.experimental.pallas import tpu as pltpu
from jax.sharding import PartitionSpec as P

BLK = 512
TILE = 256
DHALF = 3 * TILE // 2
MESH = pl.DeviceIdType.MESH

LHS = ((0, 1, 0, 1, 0, 1, 0, 1, 0, 0), (0, 1, 2, 1, 2, 2, 2, 0, 0, 0))
RHS = ((0, 0, 2, 1, 2, 2, 2, 0, 0, 0), (0, 0, 0, 1, 0, 1, 0, 1, 0, 0))
REMOTE = ((1, 1, 1, 1, 0, 0, 0, 0, 0, 0), (1, 1, 1, 1, 1, 1, 0, 0, 0, 0))
OWNER = ((0, 1, 0, 1, 0, 0, 1, 1, 0, 0), (0, 1, 0, 1, 0, 1, 1, 0, 0, 0))
SLOT = ((0, 1, 1, 0, 2, 1, 1, 2, 0, 0), (0, 1, 2, 0, 1, 2, 1, 1, 0, 0))
DIAG = tuple(int(a == b) for a, b in zip(LHS[0], RHS[0]))
N_STEPS = len(DIAG)
LAST = N_STEPS - 1
N_REMOTE = 6
LOADS = (((2, 0), 0), ((3, 1), 1), ((1, 2), 2), ((0, 3), 2), ((1, 2), 0))
FIRST = ((2, 1024), (1, 2048), (3, 4096))
N_FIRST = sum(n for n, _ in FIRST)

def dot(lhs, rhs):
    return lax.dot_general(lhs, rhs, (((1,), (1,)), ((), ())), preferred_element_type=jnp.float32)


def gram_kernel(a_ref, own, part, recv, a_buf, pair, load_sem, d2d_send, d2d_recv, ici_send, ici_recv):
    half_cols = a_ref.shape[1] // 2
    me = lax.axis_index("dp")
    chip = me // 2
    core = me % 2
    peer = chip * 2 + (1 - core)

    def pick(two):
        return two[0] if two[0] == two[1] else two[0] * (1 - chip) + two[1] * chip

    def at(table, s):
        if isinstance(s, int):
            return pick((table[0][s], table[1][s]))
        packed = [sum(v << (2 * i) for i, v in enumerate(row)) for row in table]
        return (pick(packed) >> (2 * s)) & 3

    def operand(table, s):
        last_slots = 2 * ((chip + core + LAST - s) % 2)
        return jnp.where(s < LAST - 1, at(table, s), 0) + jnp.where(s < LAST - 1, 0, 1) * (2 - last_slots)

    def load(which, lo, hi, sem):
        block, slot = LOADS[which]
        half = lo // half_cols
        return pltpu.make_async_copy(
            a_ref.at[pl.ds(pl.multiple_of(pick(block) * BLK, BLK), BLK), pl.ds(lo, hi - lo)],
            a_buf.at[slot * 2 + half, :, pl.ds(lo - half * half_cols, hi - lo)],
            load_sem.at[sem],
        )

    def first_load(base, width, c):
        col = pl.multiple_of(base + c * width, width)
        cols = pl.ds(pl.multiple_of(col % half_cols, width), width)
        return col // half_cols, cols, pl.ds(col, width)

    segments = []
    for n, width in FIRST:
        done = sum(m for m, _, _ in segments)
        base = sum(m * w for m, w, _ in segments)
        segments.append((n, width, (base, done)))

    def first_copy(width, start, c):
        half, cols, src = first_load(start[0], width, c)
        return pltpu.make_async_copy(
            a_ref.at[pl.ds(pl.multiple_of(pick(LOADS[0][0]) * BLK, BLK), BLK), src],
            a_buf.at[LOADS[0][1] * 2 + half, :, cols],
            load_sem.at[start[1] + c],
        )

    half_loads = [
        [load(which, h * half_cols, (h + 1) * half_cols, N_FIRST + 2 * which + h) for h in range(2)]
        for which in range(1, len(LOADS))
    ]
    for n, width, start in segments:
        for c in range(n):
            first_copy(width, start, c).start()
    for copy in half_loads[0] + half_loads[1]:
        copy.start()

    barrier = pltpu.get_barrier_semaphore()
    for hop in range(1, 4):
        pl.semaphore_signal(barrier, inc=1, device_id={"dp": (me + hop) % 4}, device_id_type=MESH)

    part[...] = jnp.zeros_like(part)

    def pair_copy(s):
        return pltpu.make_async_remote_copy(
            src_ref=part.at[s % 2, 1 - core],
            dst_ref=pair.at[s],
            send_sem=d2d_send.at[s],
            recv_sem=d2d_recv.at[s],
            device_id={"dp": peer},
            device_id_type=MESH,
        )

    def own_copy(s, rows):
        return pltpu.make_async_remote_copy(
            src_ref=part.at[s % 2, :, pl.ds(0, rows)],
            dst_ref=own.at[at(SLOT, s), :, pl.ds(0, rows)],
            send_sem=d2d_send.at[s],
            recv_sem=d2d_recv.at[s],
            device_id={"dp": peer},
            device_id_type=MESH,
        )

    def link_copy(s, rows):
        slot = at(SLOT, s)
        return pltpu.make_async_remote_copy(
            src_ref=pair.at[s, pl.ds(0, rows)],
            dst_ref=recv.at[slot, core, pl.ds(0, rows)],
            send_sem=ici_send.at[s],
            recv_sem=ici_recv.at[slot * 2 + core],
            device_id={"dp": (1 - chip) * 2 + at(OWNER, s)},
            device_id_type=MESH,
        )

    def link_wait(slot, half, rows):
        pltpu.make_async_remote_copy(
            src_ref=pair.at[0, pl.ds(0, rows)],
            dst_ref=recv.at[slot, half, pl.ds(0, rows)],
            send_sem=ici_send.at[0],
            recv_sem=ici_recv.at[slot * 2 + half],
            device_id={"dp": peer},
            device_id_type=MESH,
        ).wait_recv()

    def on(value, want=1):
        return pl.when(value == want)

    def send_partial(s):
        @on(at(REMOTE, s))
        def _():
            pair_copy(s).start()

        @on(jnp.where(s == LAST - 1, 1, at(REMOTE, s) * 2 + (at(OWNER, s) + core) % 2))
        def _():
            own_copy(s, BLK).start()

    def reduce_partial(s):
        @on(at(REMOTE, s))
        def _():
            pair_copy(s).wait()

            for diag, rows in ((1, DHALF), (0, BLK)):
                @on(at((DIAG, DIAG), s), diag)
                def _(rows=rows):
                    pair[s, :rows] += part[s % 2, core, :rows]
                    link_copy(s, rows).start()

        mine = at(REMOTE, s) * 2 + (at(OWNER, s) + core) % 2

        @on(mine, 0)
        def _():
            own_copy(s, BLK).wait_recv()
            own[at(SLOT, s)] += part[s % 2]

        @on(mine, 1)
        def _():
            own_copy(s, BLK).wait_send()

    def put_diag(to, low, high, add):
        for h, row, n, value in (
            (0, 0, DHALF, low[:DHALF]),
            (1, 0, BLK - DHALF, low[DHALF:]),
            (1, BLK - DHALF, TILE, high),
        ):
            to[h, row:row + n] = to[h, row:row + n] + value if add else value

    for n, width, start in segments:
        @pl.loop(0, n)
        def _(c, width=width, start=start):
            first_copy(width, start, c).wait()
            half, cols, _ = first_load(start[0], width, c)
            block = a_buf.at[half, :, cols]
            put_diag(part.at[0], dot(block[...], block[:TILE]), dot(block[TILE:], block[TILE:]), True)

    pl.semaphore_wait(barrier, 3)
    send_partial(0)

    @pl.loop(1, 2)
    def _(s):
        @pl.loop(0, 2)
        def _(h):
            @on(s * 2 + h, 2)
            def _():
                half_loads[0][0].wait()

            @on(s * 2 + h, 3)
            def _():
                half_loads[0][1].wait()

            @on(h)
            def _():
                reduce_partial(s - 1)

            value = dot(a_buf[operand(LHS, s) * 2 + h], a_buf[operand(RHS, s) * 2 + h])
            for n in range(2):
                old = jnp.where(h == 0, 0.0, part[s % 2, n])
                part[s % 2, n] = old + value[:, n * TILE:(n + 1) * TILE]

        send_partial(s)

    @pl.loop(2, N_STEPS)
    def _(s):
        for step, copies, action in (
            (2, half_loads[1], "wait"),
            (3, half_loads[2], "start"),
            (4, half_loads[2], "wait"),
            (5, half_loads[3], "start"),
            (6, half_loads[3], "wait"),
        ):
            @on(s, step)
            def _(copies=copies, action=action):
                for copy in copies:
                    getattr(copy, action)()

        diag = at((DIAG, DIAG), s)
        to = part.at[s % 2]
        left, right = operand(LHS, s) * 2, operand(RHS, s) * 2

        @on(diag)
        def _():
            for h in range(2):
                block = a_buf.at[left + h]
                put_diag(to, dot(block[...], block[:TILE]), dot(block[TILE:], block[TILE:]), h > 0)

        @on(diag, 0)
        def _():
            for h in range(2):
                value = dot(a_buf[left + h], a_buf[right + h])
                for n in range(2):
                    tile = value[:, n * TILE:(n + 1) * TILE]
                    to[n] = to[n] + tile if h else tile

        @pl.when(s < LAST)
        def _():
            reduce_partial(s - 1)
            send_partial(s)

    own_copy(LAST - 1, BLK).wait()
    for h in range(2):
        link_wait(0, h, DHALF)
        link_wait(1, h, BLK)

    @pl.when(chip == 0)
    def _():
        for h in range(2):
            link_wait(2, h, BLK)

    for s in range(N_REMOTE):
        rows = DHALF if DIAG[s] else BLK

        @on(at(REMOTE, s))
        def _(s=s, rows=rows):
            link_copy(s, rows).wait_send()


def place_kernel(own, part, recv, out_ref, done, sem):
    chip = lax.axis_index("dp") // 2
    rest = BLK - DHALF
    copies = []

    def move(slot, h, src, n, row, col):
        i = len(copies)
        copies.append(
            pltpu.make_async_copy(
                done.at[slot, h, pl.ds(src, n)], out_ref.at[0, slot, pl.ds(row, n), pl.ds(col, TILE)], sem.at[i]
            )
        )
        copies[i].start()

    def diag_sum(h, row, n):
        return own[0, h, row:row + n] + part[LAST % 2, h, row:row + n] + recv[0, h, row:row + n]

    low = [diag_sum(0, TILE, DHALF - TILE), diag_sum(1, 0, rest)]
    done[0, 0, TILE:DHALF] = low[0]
    done[0, 1, :rest] = low[1]
    done[0, 0, :TILE] = diag_sum(0, 0, TILE)
    move(0, 0, 0, DHALF, 0, 0)
    move(0, 1, 0, rest, DHALF, 0)
    done[0, 1, rest:DHALF] = diag_sum(1, rest, TILE)
    move(0, 1, rest, TILE, TILE, TILE)
    flipped = jnp.concatenate(low, axis=0).T
    done[0, 0, DHALF:] = flipped[:rest]
    done[0, 1, DHALF:] = flipped[rest:]
    move(0, 0, DHALF, rest, 0, TILE)
    move(0, 1, DHALF, rest, rest, TILE)
    for h in range(2):
        done[1, h] = own[1, h] + recv[1, h]
        move(1, h, 0, BLK, 0, h * TILE)
    for h in range(2):
        done[2, h] = jnp.where(chip == 0, own[2, h] + recv[2, h], 0.0)
        move(2, h, 0, BLK, 0, h * TILE)
    for copy in copies:
        copy.wait()


def solution(mesh):
    groups = mesh.shape["dp"]
    assert groups == 4

    def local_gram(a_local):
        n_rows, local_cols = a_local.shape
        assert n_rows == groups * BLK and local_cols == sum(n * width for n, width in FIRST)
        sums = pl.pallas_call(
            gram_kernel,
            name="gram",
            out_shape=[pltpu.VMEM((n, 2, BLK, TILE), jnp.float32) for n in (3, 2, 3)],
            in_specs=[pl.BlockSpec(memory_space=pltpu.HBM)],
            out_specs=[pl.BlockSpec(memory_space=pltpu.VMEM)] * 3,
            scratch_shapes=[
                pltpu.VMEM((6, BLK, local_cols // 2), jnp.bfloat16),
                pltpu.VMEM((N_REMOTE, BLK, TILE), jnp.float32),
                pltpu.SemaphoreType.DMA((N_FIRST + 2 * len(LOADS),)),
                pltpu.SemaphoreType.DMA((N_STEPS,)),
                pltpu.SemaphoreType.DMA((N_STEPS,)),
                pltpu.SemaphoreType.DMA((N_REMOTE,)),
                pltpu.SemaphoreType.DMA((6,)),
            ],
            compiler_params=pltpu.CompilerParams(
                collective_id=0, has_side_effects=True, vmem_limit_bytes=55 * 2**20
            ),
        )(a_local)
        return pl.pallas_call(
            place_kernel,
            name="place",
            out_shape=jax.ShapeDtypeStruct((1, 3, BLK, BLK), jnp.float32),
            in_specs=[pl.BlockSpec(memory_space=pltpu.VMEM)] * 3,
            out_specs=pl.BlockSpec(memory_space=pltpu.HBM),
            scratch_shapes=[pltpu.VMEM((3, 2, BLK, TILE), jnp.float32), pltpu.SemaphoreType.DMA((9,))],
            compiler_params=pltpu.CompilerParams(vmem_limit_bytes=8 * 2**20),
        )(*[pltpu.with_memory_space_constraint(x, pltpu.VMEM) for x in sums])

    return jax.shard_map(
        local_gram, mesh=mesh, in_specs=(P("mat", "dp"),), out_specs=P(("mat", "dp")), check_vma=False
    )
```

```python
import jax
import jax.numpy as jnp
from jax import lax
from jax.experimental import pallas as pl
from jax.experimental.pallas import tpu as pltpu
from jax.sharding import PartitionSpec as P

BLK = 512
TILE = 256
DHALF = 3 * TILE // 2
MESH = pl.DeviceIdType.MESH

LHS = ((0, 1, 0, 1, 0, 1, 0, 1, 0, 0), (0, 1, 2, 1, 2, 2, 2, 0, 0, 0))
RHS = ((0, 0, 2, 1, 2, 2, 2, 0, 0, 0), (0, 0, 0, 1, 0, 1, 0, 1, 0, 0))
REMOTE = ((1, 1, 1, 1, 0, 0, 0, 0, 0, 0), (1, 1, 1, 1, 1, 1, 0, 0, 0, 0))
OWNER = ((0, 1, 0, 1, 0, 0, 1, 1, 0, 0), (0, 1, 0, 1, 0, 1, 1, 0, 0, 0))
SLOT = ((0, 1, 1, 0, 2, 1, 1, 2, 0, 0), (0, 1, 2, 0, 1, 2, 1, 1, 0, 0))
DIAG = tuple(int(a == b) for a, b in zip(LHS[0], RHS[0]))
N_STEPS = len(DIAG)
LAST = N_STEPS - 1
N_REMOTE = 6
LOADS = (((2, 0), 0), ((3, 1), 1), ((1, 2), 2), ((0, 3), 2), ((1, 2), 0))
FIRST = ((2, 1024), (1, 2048), (3, 4096))
N_FIRST = sum(n for n, _ in FIRST)

def dot(lhs, rhs):
    return lax.dot_general(lhs, rhs, (((1,), (1,)), ((), ())), preferred_element_type=jnp.float32)


def gram_kernel(a_ref, own, part, recv, a_buf, pair, load_sem, d2d_send, d2d_recv, ici_send, ici_recv):
    half_cols = a_ref.shape[1] // 2
    me = lax.axis_index("dp")
    chip = me // 2
    core = me % 2
    peer = chip * 2 + (1 - core)

    def pick(two):
        return two[0] if two[0] == two[1] else two[0] * (1 - chip) + two[1] * chip

    def at(table, s):
        if isinstance(s, int):
            return pick((table[0][s], table[1][s]))
        packed = [sum(v << (2 * i) for i, v in enumerate(row)) for row in table]
        return (pick(packed) >> (2 * s)) & 3

    def operand(table, s):
        last_slots = 2 * ((chip + core + LAST - s) % 2)
        return jnp.where(s < LAST - 1, at(table, s), 0) + jnp.where(s < LAST - 1, 0, 1) * (2 - last_slots)

    def load(which, lo, hi, sem):
        block, slot = LOADS[which]
        half = lo // half_cols
        return pltpu.make_async_copy(
            a_ref.at[pl.ds(pl.multiple_of(pick(block) * BLK, BLK), BLK), pl.ds(lo, hi - lo)],
            a_buf.at[slot * 2 + half, :, pl.ds(lo - half * half_cols, hi - lo)],
            load_sem.at[sem],
        )

    def first_load(base, width, c):
        col = pl.multiple_of(base + c * width, width)
        cols = pl.ds(pl.multiple_of(col % half_cols, width), width)
        return col // half_cols, cols, pl.ds(col, width)

    segments = []
    for n, width in FIRST:
        done = sum(m for m, _, _ in segments)
        base = sum(m * w for m, w, _ in segments)
        segments.append((n, width, (base, done)))

    def first_copy(width, start, c):
        half, cols, src = first_load(start[0], width, c)
        return pltpu.make_async_copy(
            a_ref.at[pl.ds(pl.multiple_of(pick(LOADS[0][0]) * BLK, BLK), BLK), src],
            a_buf.at[LOADS[0][1] * 2 + half, :, cols],
            load_sem.at[start[1] + c],
        )

    half_loads = [
        [load(which, h * half_cols, (h + 1) * half_cols, N_FIRST + 2 * which + h) for h in range(2)]
        for which in range(1, len(LOADS))
    ]
    for n, width, start in segments:
        for c in range(n):
            first_copy(width, start, c).start()
    for copy in half_loads[0] + half_loads[1]:
        copy.start()

    barrier = pltpu.get_barrier_semaphore()
    for hop in range(1, 4):
        pl.semaphore_signal(barrier, inc=1, device_id={"dp": (me + hop) % 4}, device_id_type=MESH)

    part[...] = jnp.zeros_like(part)

    def pair_copy(s):
        return pltpu.make_async_remote_copy(
            src_ref=part.at[s % 2, 1 - core],
            dst_ref=pair.at[s],
            send_sem=d2d_send.at[s],
            recv_sem=d2d_recv.at[s],
            device_id={"dp": peer},
            device_id_type=MESH,
        )

    def own_copy(s, rows):
        return pltpu.make_async_remote_copy(
            src_ref=part.at[s % 2, :, pl.ds(0, rows)],
            dst_ref=own.at[at(SLOT, s), :, pl.ds(0, rows)],
            send_sem=d2d_send.at[s],
            recv_sem=d2d_recv.at[s],
            device_id={"dp": peer},
            device_id_type=MESH,
        )

    def link_copy(s, rows):
        slot = at(SLOT, s)
        return pltpu.make_async_remote_copy(
            src_ref=pair.at[s, pl.ds(0, rows)],
            dst_ref=recv.at[slot, core, pl.ds(0, rows)],
            send_sem=ici_send.at[s],
            recv_sem=ici_recv.at[slot * 2 + core],
            device_id={"dp": (1 - chip) * 2 + at(OWNER, s)},
            device_id_type=MESH,
        )

    def link_wait(slot, half, rows):
        pltpu.make_async_remote_copy(
            src_ref=pair.at[0, pl.ds(0, rows)],
            dst_ref=recv.at[slot, half, pl.ds(0, rows)],
            send_sem=ici_send.at[0],
            recv_sem=ici_recv.at[slot * 2 + half],
            device_id={"dp": peer},
            device_id_type=MESH,
        ).wait_recv()

    def on(value, want=1):
        return pl.when(value == want)

    def send_partial(s):
        @on(at(REMOTE, s))
        def _():
            pair_copy(s).start()

        @on(jnp.where(s == LAST - 1, 1, at(REMOTE, s) * 2 + (at(OWNER, s) + core) % 2))
        def _():
            own_copy(s, BLK).start()

    def reduce_partial(s):
        @on(at(REMOTE, s))
        def _():
            pair_copy(s).wait()

            for diag, rows in ((1, DHALF), (0, BLK)):
                @on(at((DIAG, DIAG), s), diag)
                def _(rows=rows):
                    pair[s, :rows] += part[s % 2, core, :rows]
                    link_copy(s, rows).start()

        mine = at(REMOTE, s) * 2 + (at(OWNER, s) + core) % 2

        @on(mine, 0)
        def _():
            own_copy(s, BLK).wait_recv()
            own[at(SLOT, s)] += part[s % 2]

        @on(mine, 1)
        def _():
            own_copy(s, BLK).wait_send()

    def put_diag(to, low, high, add):
        for h, row, n, value in (
            (0, 0, DHALF, low[:DHALF]),
            (1, 0, BLK - DHALF, low[DHALF:]),
            (1, BLK - DHALF, TILE, high),
        ):
            to[h, row:row + n] = to[h, row:row + n] + value if add else value

    for n, width, start in segments:
        @pl.loop(0, n)
        def _(c, width=width, start=start):
            first_copy(width, start, c).wait()
            half, cols, _ = first_load(start[0], width, c)
            block = a_buf.at[half, :, cols]
            put_diag(part.at[0], dot(block[...], block[:TILE]), dot(block[TILE:], block[TILE:]), True)

    pl.semaphore_wait(barrier, 3)
    send_partial(0)

    @pl.loop(1, 2)
    def _(s):
        @pl.loop(0, 2)
        def _(h):
            @on(s * 2 + h, 2)
            def _():
                half_loads[0][0].wait()

            @on(s * 2 + h, 3)
            def _():
                half_loads[0][1].wait()

            @on(h)
            def _():
                reduce_partial(s - 1)

            value = dot(a_buf[operand(LHS, s) * 2 + h], a_buf[operand(RHS, s) * 2 + h])
            for n in range(2):
                old = jnp.where(h == 0, 0.0, part[s % 2, n])
                part[s % 2, n] = old + value[:, n * TILE:(n + 1) * TILE]

        send_partial(s)

    @pl.loop(2, N_STEPS)
    def _(s):
        for step, copies, action in (
            (2, half_loads[1], "wait"),
            (3, half_loads[2], "start"),
            (4, half_loads[2], "wait"),
            (5, half_loads[3], "start"),
            (6, half_loads[3], "wait"),
        ):
            @on(s, step)
            def _(copies=copies, action=action):
                for copy in copies:
                    getattr(copy, action)()

        diag = at((DIAG, DIAG), s)
        to = part.at[s % 2]
        left, right = operand(LHS, s) * 2, operand(RHS, s) * 2

        @on(diag)
        def _():
            for h in range(2):
                block = a_buf.at[left + h]
                put_diag(to, dot(block[...], block[:TILE]), dot(block[TILE:], block[TILE:]), h > 0)

        @on(diag, 0)
        def _():
            for h in range(2):
                value = dot(a_buf[left + h], a_buf[right + h])
                for n in range(2):
                    tile = value[:, n * TILE:(n + 1) * TILE]
                    to[n] = to[n] + tile if h else tile

        @pl.when(s < LAST)
        def _():
            reduce_partial(s - 1)
            send_partial(s)

    own_copy(LAST - 1, BLK).wait()
    for h in range(2):
        link_wait(0, h, DHALF)
        link_wait(1, h, BLK)

    @pl.when(chip == 0)
    def _():
        for h in range(2):
            link_wait(2, h, BLK)

    for s in range(N_REMOTE):
        rows = DHALF if DIAG[s] else BLK

        @on(at(REMOTE, s))
        def _(s=s, rows=rows):
            link_copy(s, rows).wait_send()


def place_kernel(own, part, recv, out_ref, done, sem):
    chip = lax.axis_index("dp") // 2
    rest = BLK - DHALF
    copies = []

    def move(slot, h, src, n, row, col):
        i = len(copies)
        copies.append(
            pltpu.make_async_copy(
                done.at[slot, h, pl.ds(src, n)], out_ref.at[0, slot, pl.ds(row, n), pl.ds(col, TILE)], sem.at[i]
            )
        )
        copies[i].start()

    def diag_sum(h, row, n):
        return own[0, h, row:row + n] + part[LAST % 2, h, row:row + n] + recv[0, h, row:row + n]

    for h in range(2):
        done[1, h] = own[1, h] + recv[1, h]
        move(1, h, 0, BLK, 0, h * TILE)
    for h in range(2):
        done[2, h] = jnp.where(chip == 0, own[2, h] + recv[2, h], 0.0)
        move(2, h, 0, BLK, 0, h * TILE)
    low = [diag_sum(0, TILE, DHALF - TILE), diag_sum(1, 0, rest)]
    done[0, 0, TILE:DHALF] = low[0]
    done[0, 1, :rest] = low[1]
    done[0, 0, :TILE] = diag_sum(0, 0, TILE)
    move(0, 0, 0, DHALF, 0, 0)
    move(0, 1, 0, rest, DHALF, 0)
    done[0, 1, rest:DHALF] = diag_sum(1, rest, TILE)
    move(0, 1, rest, TILE, TILE, TILE)
    flipped = jnp.concatenate(low, axis=0).T
    done[0, 0, DHALF:] = flipped[:rest]
    done[0, 1, DHALF:] = flipped[rest:]
    move(0, 0, DHALF, rest, 0, TILE)
    move(0, 1, DHALF, rest, rest, TILE)
    for copy in copies:
        copy.wait()


def solution(mesh):
    groups = mesh.shape["dp"]
    assert groups == 4

    def local_gram(a_local):
        n_rows, local_cols = a_local.shape
        assert n_rows == groups * BLK and local_cols == sum(n * width for n, width in FIRST)
        sums = pl.pallas_call(
            gram_kernel,
            name="gram",
            out_shape=[pltpu.VMEM((n, 2, BLK, TILE), jnp.float32) for n in (3, 2, 3)],
            in_specs=[pl.BlockSpec(memory_space=pltpu.HBM)],
            out_specs=[pl.BlockSpec(memory_space=pltpu.VMEM)] * 3,
            scratch_shapes=[
                pltpu.VMEM((6, BLK, local_cols // 2), jnp.bfloat16),
                pltpu.VMEM((N_REMOTE, BLK, TILE), jnp.float32),
                pltpu.SemaphoreType.DMA((N_FIRST + 2 * len(LOADS),)),
                pltpu.SemaphoreType.DMA((N_STEPS,)),
                pltpu.SemaphoreType.DMA((N_STEPS,)),
                pltpu.SemaphoreType.DMA((N_REMOTE,)),
                pltpu.SemaphoreType.DMA((6,)),
            ],
            compiler_params=pltpu.CompilerParams(
                collective_id=0, has_side_effects=True, vmem_limit_bytes=55 * 2**20
            ),
        )(a_local)
        return pl.pallas_call(
            place_kernel,
            name="place",
            out_shape=jax.ShapeDtypeStruct((1, 3, BLK, BLK), jnp.float32),
            in_specs=[pl.BlockSpec(memory_space=pltpu.VMEM)] * 3,
            out_specs=pl.BlockSpec(memory_space=pltpu.HBM),
            scratch_shapes=[pltpu.VMEM((3, 2, BLK, TILE), jnp.float32), pltpu.SemaphoreType.DMA((9,))],
            compiler_params=pltpu.CompilerParams(vmem_limit_bytes=8 * 2**20),
        )(*[pltpu.with_memory_space_constraint(x, pltpu.VMEM) for x in sums])

    return jax.shard_map(
        local_gram, mesh=mesh, in_specs=(P("mat", "dp"),), out_specs=P(("mat", "dp")), check_vma=False
    )
```
